32 devices in a mesh: tm: 8 (over z, core), block: 4 (over y, x).
Axes of the slice: x: 2, y: 2, z: 4, core: 2. Of those that a mesh axis runs over, the one named last changes fastest.
Arguments:
- state: float32 [16, 4, 256, 512], P('tm', None, None, 'block'), may hold values from -6 to 6
- far_field: float32 [16, 4, 512], P('tm', None, 'block'), may hold values from -6 to 6
- face_index: int32 [16, 512], P('tm', 'block'), may hold values from 0 to 255, as said below
- face_weight: float32 [16, 4, 512], P('tm', None, 'block'), may hold values from 0.05 to 0.45
- mean_flow: float32 [2, 2], replicated, may hold values from -0.6 to 0.6
Outputs:
- new_state: float32 [16, 4, 256, 512], P('tm', None, None, 'block')
The draws below stay inside these ranges and needn't reach their ends.
Inputs may be any that keep to these rules, and one draw needn't show every extreme that they name: `face_index`: each face's index points into the opposite row's 2 * 128 interface faces laid end to end; the 4 faces read wrap around that cycle. At each level, the faces of one blade row take distinct first indices, every face of the opposite row exactly once.
All inputs are finite; a program needn't handle non-finite values.
Results may differ from the reference program's by a relative error of at most 0.00016.
Values sent between devices are 32-bit elements; how exact they have to be, the bound alone decides.
A program may use at most 64 MiB of HBM per device.

```python
import jax
import jax.numpy as jnp
from jax import lax

NT = 16
NI = 256
NJ = 128
K = 4
BLOCKS = 4
HALF = 2


def draw_face_index(key, part):
    base = jax.random.fold_in(key, 7)
    cycle_size = HALF * NJ
    level_keys = jax.random.split(base, NT * 2)
    orders = jax.vmap(lambda single: jax.random.permutation(single, cycle_size))(level_keys)
    column = jnp.arange(BLOCKS * NJ)
    block_number = column // NJ
    side = block_number // HALF
    place = block_number % HALF * NJ + column % NJ
    flat = orders.reshape(NT, 2 * cycle_size)
    return jnp.take(flat, side * cycle_size + place, axis=1).astype(jnp.int32)


def block_levels(stream_key, shape, cuts, smallest, top_value):
    level = 1.0
    for axis_at, blocks in cuts:
        draws = jax.random.uniform(jax.random.fold_in(jax.random.fold_in(stream_key, 6), axis_at), (blocks,), jnp.float32, smallest / len(cuts), top_value / len(cuts))
        level = level * jnp.repeat(jnp.exp(draws), shape[axis_at] // blocks).reshape((-1,) + (1,) * (len(shape) - 1 - axis_at))
    return level


def centred(own_key, extent, deviation, limit, cuts=(), held_as=jnp.bfloat16):
    factor_of = block_levels(own_key, extent, cuts, -0.22, 0.18) if cuts else 1.0
    entries = jax.random.normal(own_key, extent, jnp.float32) * deviation * factor_of
    return jnp.minimum(jnp.maximum(entries, -limit), limit).astype(held_as)


def setup_inputs(seed: int = 0) -> dict:
    keys = jax.random.split(jax.random.key(seed), 6)
    state = centred(keys[0], (NT, 4, NI, BLOCKS * NJ), 1.0, 6.0, ((0, 8), (3, 4)), jnp.float32)
    far_field = centred(keys[1], (NT, 4, BLOCKS * NJ), 1.0, 6.0, ((0, 8), (2, 4)), jnp.float32)
    face_index = draw_face_index(jax.random.fold_in(keys[5], 71), 0)
    face_weight = jnp.clip(0.05 + 0.39999999 * jax.random.uniform(keys[3], (NT, K, BLOCKS * NJ), jnp.float32) ** block_levels(keys[3], (NT, K, BLOCKS * NJ), ((0, 8), (2, 4)), -0.2, 0.2), 0.05, 0.45)
    mean_flow = jnp.clip(jax.random.uniform(keys[4], (2, 2), jnp.float32, -0.6, 0.6), -0.6, 0.6)
    return {"state": state, "far_field": far_field, "face_index": face_index, "face_weight": face_weight, "mean_flow": mean_flow}


SECTION_FACTORS = (0.075, 0.05, 0.1125, 0.15, 0.3)
OMEGA = 1.0
DISSIPATION = 0.2


def derivative_matrix(count):
    index = jnp.arange(count)
    offsets = index[:, None] - index[None, :]
    angle = jnp.pi * offsets.astype(jnp.float32) / count
    parity_sign = 1.0 - 2.0 * (offsets % 2).astype(jnp.float32)
    safe_angle = jnp.where(offsets == 0, 0.5 * jnp.pi, angle)
    cotangent = jnp.cos(safe_angle) / jnp.sin(safe_angle)
    return jnp.where(offsets == 0, 0.0, 0.5 * parity_sign * cotangent).astype(jnp.float32)


def interpolate(faces, table, weight):
    cycle_size = faces.shape[2]
    total = jnp.zeros(faces.shape, jnp.float32)
    for offset in range(weight.shape[1]):
        source = ((table + offset) % cycle_size).astype(jnp.int32)
        picked = jnp.take_along_axis(faces, jnp.broadcast_to(source[:, None, :], faces.shape), axis=2)
        total = total + weight[:, offset][:, None, :] * picked
    return total


def residual(field, lower_ghost, upper_ghost, lower_col, upper_col, speed_u, speed_v):
    padded_i = jnp.concatenate([lower_ghost[:, :, None], field, upper_ghost[:, :, None]], axis=2)
    padded_j = jnp.concatenate([lower_col, field, upper_col], axis=3)
    diff_i = padded_i[:, :, 2:] - padded_i[:, :, :-2]
    diff_j = padded_j[..., 2:] - padded_j[..., :-2]
    laplace = (padded_i[:, :, 2:] - 2.0 * field + padded_i[:, :, :-2]) + (padded_j[..., 2:] - 2.0 * field + padded_j[..., :-2])
    flux_i = jnp.stack([speed_u * diff_i[:, 0] + diff_i[:, 1], speed_u * diff_i[:, 1] + diff_i[:, 3],
                        speed_u * diff_i[:, 2], speed_u * diff_i[:, 3] + diff_i[:, 1]], axis=1)
    flux_j = jnp.stack([speed_v * diff_j[:, 0] + diff_j[:, 2], speed_v * diff_j[:, 1],
                        speed_v * diff_j[:, 2] + diff_j[:, 3], speed_v * diff_j[:, 3] + diff_j[:, 2]], axis=1)
    return 0.5 * (flux_i + flux_j) - DISSIPATION * laplace


def reference(state, far_field, face_index, face_weight, mean_flow):
    half = BLOCKS // 2
    spectral = derivative_matrix(NT)
    far_rows = far_field.reshape(NT, 4, 2, half * NJ)
    tables = face_index.reshape(NT, 2, half * NJ)
    weights = face_weight.reshape(NT, K, 2, half * NJ)
    field = state
    for factor in SECTION_FACTORS:
        blocked = field.reshape(NT, 4, NI, 2, half * NJ)
        pieces = []
        for side in (0, 1):
            part = blocked[:, :, :, side]
            other = blocked[:, :, :, 1 - side]
            other_face = other[:, :, 0] if side == 0 else other[:, :, NI - 1]
            ghost = interpolate(other_face, tables[:, side], weights[:, :, side])
            far_side = far_rows[:, :, side]
            if side == 0:
                lower_ghost, upper_ghost = far_side, ghost
            else:
                lower_ghost, upper_ghost = ghost, far_side
            flux = residual(part, lower_ghost, upper_ghost, part[..., -1:], part[..., :1],
                            mean_flow[side, 0], mean_flow[side, 1])
            pieces.append(flux)
        flux_all = jnp.stack(pieces, axis=3).reshape(NT, 4, NI, BLOCKS * NJ)
        deriv = jnp.einsum('nm,mvij->nvij', spectral, field, precision=lax.Precision.HIGHEST)
        field = state - factor * (flux_all + OMEGA * deriv)
    return field
```

```python
import functools
import math

import jax
import jax.numpy as jnp
from jax import lax
from jax.experimental import pallas as pl
from jax.experimental.pallas import tpu as pltpu
from jax.sharding import PartitionSpec as P

SECTION_FACTORS = (0.075, 0.05, 0.1125, 0.15, 0.3)
OMEGA = 1.0
DISSIPATION = 0.2
PAD = 8
MESH = pl.DeviceIdType.MESH


def split_coefficients(count):
    half = count // 2
    d = [0.0] + [0.5 * (-1) ** k / math.tan(math.pi * k / count) for k in range(1, half)] + [0.0]
    even = [0.5 * OMEGA * (d[m] - d[half - m]) for m in range(half)]
    odd = [0.5 * OMEGA * (d[m] + d[half - m]) for m in range(half)]
    even[0] = odd[0] = 0.0
    return even, odd


def time_term(q, even, odd):
    half = len(q) // 2
    quarter = half // 2
    e = [q[n] + q[n + half] for n in range(half)]
    o = [q[n] - q[n + half] for n in range(half)]

    def odd_at(n):
        return (o[n % half], -1.0 if (n // half) % 2 else 1.0)

    low, high = [], []
    for n in range(half):
        ev = None
        od = None
        for m in range(1, quarter):
            term = even[m] * (e[(n - m) % half] - e[(n + m) % half])
            ev = term if ev is None else ev + term
            (a, sa), (b, sb) = odd_at(n - m), odd_at(n + m)
            pair = a - b if sa == sb else a + b
            term = (odd[m] * sa) * pair
            od = term if od is None else od + term
        a, sa = odd_at(n - quarter)
        od = od + (odd[quarter] * sa) * a
        low.append(ev + od)
        high.append(ev - od)
    return low + high


def kernel(dims, state, far, fidx, fw, mf, out, x0, qa, qb, ef, el, rl, ru, cs, cl, cu,
           face, ff, wts, fi, lane_ix, blk_ix, ww, gh,
           in_s, in_r, out_s, out_r, p_s, p_r, h_s, h_r, f_s, f_r, loc):
    tm_n, half, L, R, K = dims
    NT = tm_n * L
    cycle = half * 128
    tiles = R // 8
    nsec = len(SECTION_FACTORS)
    me = lax.axis_index("tm")
    blk = lax.axis_index("block")
    side = lax.div(blk, half)
    place = lax.rem(blk, half)
    row0 = side * half
    lower_b = row0 + lax.rem(place + half - 1, half)
    upper_b = row0 + lax.rem(place + 1, half)
    other0 = (1 - side) * half
    step = 1 - 2 * side
    is_last = me == tm_n - 1
    is_far = me == 0
    rchunk = side * (tm_n - 1) + step * me
    has_lower = rchunk > 0
    has_upper = rchunk < tm_n - 1
    ghost_row = jnp.where(side == 0, PAD + R, PAD - 1)
    far_row = jnp.where(side == 0, PAD - 1, PAD + R)

    def rc(src, dst, ss, rs, dev):
        return pltpu.make_async_remote_copy(src_ref=src, dst_ref=dst, send_sem=ss, recv_sem=rs,
                                            device_id=dev, device_id_type=MESH)

    def rows(p):
        return pl.ds(pl.multiple_of((side * (tm_n - 1) + step * p) * R, R), R)

    def lev(p):
        return pl.ds(p * L, L)

    def peer(t):
        return lax.rem(me + t, tm_n)

    bar = pltpu.get_barrier_semaphore()

    @pl.loop(1, tm_n)
    def _(t):
        pl.semaphore_signal(bar, inc=1, device_id={"tm": peer(t)}, device_id_type=MESH)

    pl.semaphore_signal(bar, inc=1, device_id={"block": lower_b}, device_id_type=MESH)
    pl.semaphore_signal(bar, inc=1, device_id={"block": upper_b}, device_id_type=MESH)

    @pl.when(is_last)
    def _():
        for h in range(half):
            pl.semaphore_signal(bar, inc=1, device_id={"block": other0 + h}, device_id_type=MESH)

    own = pltpu.make_async_copy(state.at[:, :, rows(me)], x0.at[lev(me)], loc.at[0])
    own.start()
    pl.semaphore_wait(bar, tm_n + 1 + jnp.where(is_last, half, 0))

    def in_copy(p, src_tm):
        return rc(state.at[:, :, rows(p)], x0.at[lev(src_tm)], in_s.at[p], in_r.at[src_tm], {"tm": p})

    @pl.loop(1, tm_n)
    def _(t):
        p = peer(t)
        in_copy(p, me).start()

    def far_copy(src_tm):
        return rc(far, ff.at[lev(src_tm)], p_s.at[0], p_r.at[0, src_tm], {"tm": 0})

    def wt_copy(src_tm):
        return rc(fw, wts.at[lev(src_tm)], p_s.at[1], p_r.at[1, src_tm], {"tm": tm_n - 1})

    def ix_copy(src_tm):
        return rc(fidx, fi.at[src_tm], p_s.at[2], p_r.at[2, src_tm], {"tm": tm_n - 1})

    own_far = pltpu.make_async_copy(far, ff.at[lev(me)], loc.at[1])
    own_wt = pltpu.make_async_copy(fw, wts.at[lev(me)], loc.at[2])
    own_ix = pltpu.make_async_copy(fidx, fi.at[me], loc.at[3])

    @pl.when(is_far)
    def _():
        own_far.start()

    @pl.when(jnp.logical_not(is_far))
    def _():
        far_copy(me).start()

    @pl.when(is_last)
    def _():
        own_wt.start()
        own_ix.start()

    @pl.when(jnp.logical_not(is_last))
    def _():
        wt_copy(me).start()
        ix_copy(me).start()

    lane = lax.broadcasted_iota(jnp.int32, (8, 128), 1)
    sub = lax.broadcasted_iota(jnp.int32, (8, 128), 0)

    def pack(acc, value, k):
        return jnp.where((lane == k) | (lane == k - 1), pltpu.roll(value, k, 1), acc)

    def key(l, v):
        return 2 * (4 * l + v) + 1

    def halo_copies(s):
        low = rc(ef.at[s], ru.at[s], h_s.at[s, 0], h_r.at[s, 0], {"tm": me - step})
        up = rc(el.at[s], rl.at[s], h_s.at[s, 1], h_r.at[s, 1], {"tm": me + step})
        jl = rc(cs.at[s], cu.at[s], h_s.at[s, 2], h_r.at[s, 2], {"block": lower_b})
        ju = rc(cs.at[s], cl.at[s], h_s.at[s, 3], h_r.at[s, 3], {"block": upper_b})
        return low, up, jl, ju

    def face_copy(s, h, edge):
        return rc(edge.at[s], face.at[s, place], f_s.at[s, h], f_r.at[s, place], {"block": other0 + h})

    def face_wait(s, h):
        return rc(ef.at[s], face.at[s, h], f_s.at[s, h], f_r.at[s, h], {"block": other0 + h})

    def send_halos(s):
        low, up, jl, ju = halo_copies(s)

        @pl.when(is_last & (side == 0))
        def _():
            for h in range(half):
                face_copy(s, h, el).start()

        @pl.when(is_last & (side == 1))
        def _():
            for h in range(half):
                face_copy(s, h, ef).start()

        @pl.when(has_lower)
        def _():
            low.start()

        @pl.when(has_upper)
        def _():
            up.start()

        jl.start()
        ju.start()

    def take_level(l, accs):
        accs = list(accs)
        for v in range(4):
            for a in range(tiles):
                value = x0[l, v, pl.ds(8 * a, 8)]
                qa[l, v, pl.ds(PAD + 8 * a, 8)] = value
                accs[a] = pack(accs[a], value, key(l, v))
                if a == 0:
                    ef[0, pl.ds(4 * l + v, 1)] = value[0:1]
                if a == tiles - 1:
                    el[0, pl.ds(4 * l + v, 1)] = value[7:8]
        return tuple(accs)

    own.wait()
    accs = tuple(jnp.zeros((8, 128), jnp.float32) for _ in range(tiles))
    accs = lax.fori_loop(0, L, lambda j, c: take_level(me * L + j, c), accs)

    def arrive(t, c):
        p = peer(t)
        in_copy(p, p).wait_recv()
        return lax.fori_loop(0, L, lambda j, d: take_level(p * L + j, d), c)

    accs = lax.fori_loop(1, tm_n, arrive, accs)
    for a in range(tiles):
        cs[0, pl.ds(8 * a, 8)] = accs[a]
    send_halos(0)

    @pl.when(is_far)
    def _():
        own_far.wait()

        @pl.loop(1, tm_n)
        def _(p):
            far_copy(p).wait_recv()

        @pl.loop(0, NT)
        def _(l):
            for v in range(4):
                row = ff[l, pl.ds(v, 1)]
                qa[l, v, pl.ds(far_row, 1)] = row
                qb[l, v, pl.ds(far_row, 1)] = row

    @pl.when(is_last)
    def _():
        own_wt.wait()
        own_ix.wait()

        @pl.loop(0, tm_n - 1)
        def _(p):
            wt_copy(p).wait_recv()
            ix_copy(p).wait_recv()

        @pl.loop(0, NT // 2)
        def _(m):
            def ix(l):
                return jnp.broadcast_to(fi[lax.div(l, L), pl.ds(lax.rem(l, L), 1)], (8, 128))

            def wt(l, k):
                return jnp.broadcast_to(wts[l, pl.ds(k, 1)], (8, 128))

            start = jnp.where(sub < 4, ix(2 * m), ix(2 * m + 1))
            at = pl.ds(8 * m, 8)
            for k in range(K):
                src = start + k
                src = jnp.where(src >= cycle, src - cycle, src)
                lane_ix[k, at] = jnp.bitwise_and(src, 127)
                blk_ix[k, at] = lax.shift_right_logical(src, 7)
                ww[k, at] = jnp.where(sub < 4, wt(2 * m, k), wt(2 * m + 1, k))

    even, odd = split_coefficients(NT)
    speed_u = jnp.where(side == 0, mf[0, 0], mf[1, 0])
    speed_v = jnp.where(side == 0, mf[0, 1], mf[1, 1])
    odd_lane = jnp.bitwise_and(lane, 1) == 1
    edge_lane = {0: lane == 0, 127: lane == 127}

    def install(dst, src, at):
        @pl.loop(0, NT)
        def _(l):
            for v in range(4):
                dst[l, v, pl.ds(at, 1)] = src[pl.ds(4 * l + v, 1)]

    def out_copy(q, p, src_tm):
        return rc(q.at[lev(p), :, pl.ds(PAD, R)], out.at[:, :, rows(src_tm)],
                  out_s.at[p], out_r.at[src_tm], {"tm": p})

    for s, factor in enumerate(SECTION_FACTORS):
        q, nq = (qa, qb) if s % 2 == 0 else (qb, qa)
        final = s == nsec - 1

        @pl.loop(0, 4)
        def _(v):
            @pl.loop(0, tiles)
            def _(a):
                at = pl.ds(pl.multiple_of(PAD + 8 * a, 8), 8)
                terms = time_term([q[l, v, at] for l in range(NT)], even, odd)
                for l in range(NT):
                    nq[l, v, at] = terms[l]

        low, up, jl, ju = halo_copies(s)

        @pl.when(has_lower)
        def _():
            up.wait_recv()
            install(q, rl.at[s], PAD - 1)

        @pl.when(has_upper)
        def _():
            low.wait_recv()
            install(q, ru.at[s], PAD + R)

        jl.wait_recv()
        ju.wait_recv()

        @pl.when(is_last)
        def _():
            for h in range(half):
                face_wait(s, h).wait_recv()

            @pl.loop(0, NT // 2)
            def _(m):
                at = pl.ds(8 * m, 8)
                total = jnp.zeros((8, 128), jnp.float32)
                for k in range(K):
                    picked = jnp.zeros((8, 128), jnp.float32)
                    for h in range(half):
                        got = jnp.take_along_axis(face[s, h, at], lane_ix[k, at], axis=1)
                        picked = jnp.where(blk_ix[k, at] == h, got, picked)
                    total = total + ww[k, at] * picked
                gh[at] = total

            install(q, gh, ghost_row)

        mixed = []
        for a in range(tiles):
            at = pl.ds(8 * a, 8)
            mixed.append(jnp.where(odd_lane, pltpu.roll(cl[s, at], 1, 1), pltpu.roll(cu[s, at], 127, 1)))

        def level(l, accs):
            accs = list(accs)
            for a in range(tiles):
                base = PAD + 8 * a
                di, dj, lap = [], [], []
                for v in range(4):
                    x = q[l, v, pl.ds(base, 8)]
                    upx = q[l, v, pl.ds(base + 1, 8)]
                    dnx = q[l, v, pl.ds(base - 1, 8)]
                    border = pltpu.roll(mixed[a], 128 - key(l, v), 1)
                    left = jnp.where(edge_lane[0], border, pltpu.roll(x, 1, 1))
                    right = jnp.where(edge_lane[127], border, pltpu.roll(x, 127, 1))
                    di.append(upx - dnx)
                    dj.append(right - left)
                    lap.append(DISSIPATION * ((upx + dnx) + (right + left) - 4.0 * x))
                flux = [
                    speed_u * di[0] + di[1] + (speed_v * dj[0] + dj[2]),
                    speed_u * di[1] + di[3] + speed_v * dj[1],
                    speed_u * di[2] + (speed_v * dj[2] + dj[3]),
                    speed_u * di[3] + di[1] + (speed_v * dj[3] + dj[2]),
                ]
                for v in range(4):
                    term = nq[l, v, pl.ds(base, 8)]
                    new = x0[l, v, pl.ds(8 * a, 8)] - factor * (0.5 * flux[v] - lap[v] + term)
                    nq[l, v, pl.ds(base, 8)] = new
                    if not final:
                        accs[a] = pack(accs[a], new, key(l, v))
                        if a == 0:
                            ef[s + 1, pl.ds(4 * l + v, 1)] = new[0:1]
                        if a == tiles - 1:
                            el[s + 1, pl.ds(4 * l + v, 1)] = new[7:8]
            return tuple(accs)

        if not final:
            accs = tuple(jnp.zeros((8, 128), jnp.float32) for _ in range(tiles))
            accs = lax.fori_loop(0, NT, level, accs)
            for a in range(tiles):
                cs[s + 1, pl.ds(8 * a, 8)] = accs[a]
            send_halos(s + 1)
        else:
            def finish(t, c):
                p = peer(t)
                lax.fori_loop(0, L, lambda j, d: (level(p * L + j, ()), d)[1], 0)

                @pl.when(t < tm_n)
                def _():
                    out_copy(nq, p, me).start()

                return c

            lax.fori_loop(1, tm_n + 1, finish, 0)
            own_out = pltpu.make_async_copy(nq.at[lev(me), :, pl.ds(PAD, R)], out.at[:, :, rows(me)], loc.at[4])
            own_out.start()

            @pl.loop(1, tm_n)
            def _(t):
                p = peer(t)
                out_copy(nq, p, p).wait_recv()

            own_out.wait()

            @pl.loop(1, tm_n)
            def _(t):
                p = peer(t)
                out_copy(nq, p, me).wait_send()

    @pl.loop(1, tm_n)
    def _(t):
        p = peer(t)
        in_copy(p, me).wait_send()

    @pl.when(jnp.logical_not(is_far))
    def _():
        far_copy(me).wait_send()

    @pl.when(jnp.logical_not(is_last))
    def _():
        wt_copy(me).wait_send()
        ix_copy(me).wait_send()

    for s in range(nsec):
        low, up, jl, ju = halo_copies(s)

        @pl.when(has_lower)
        def _():
            low.wait_send()

        @pl.when(has_upper)
        def _():
            up.wait_send()

        jl.wait_send()
        ju.wait_send()

        @pl.when(is_last)
        def _():
            for h in range(half):
                face_wait(s, h).wait_send()


def shards(dims, state, far_field, face_index, face_weight, mean_flow):
    tm_n, half = dims
    L, _, rows, width = state.shape
    K = face_weight.shape[1]
    R = rows // tm_n
    NT = L * tm_n
    assert width == 128 and NT % 4 == 0 and R % 8 == 0 and 8 * NT <= width
    n = len(SECTION_FACTORS)
    f32 = jnp.float32
    hbm = pl.BlockSpec(memory_space=pl.ANY)
    dma = pltpu.SemaphoreType.DMA
    V = pltpu.VMEM
    return pl.pallas_call(
        functools.partial(kernel, (tm_n, half, L, R, K)),
        out_shape=jax.ShapeDtypeStruct(state.shape, f32),
        in_specs=[hbm, hbm, hbm, hbm, pl.BlockSpec(memory_space=pltpu.SMEM)],
        out_specs=hbm,
        scratch_shapes=[
            V((NT, 4, R, width), f32),
            V((NT, 4, R + 2 * PAD, width), f32),
            V((NT, 4, R + 2 * PAD, width), f32),
            V((n, 4 * NT, width), f32),
            V((n, 4 * NT, width), f32),
            V((n, 4 * NT, width), f32),
            V((n, 4 * NT, width), f32),
            V((n, R, width), f32),
            V((n, R, width), f32),
            V((n, R, width), f32),
            V((n, half, 4 * NT, width), f32),
            V((NT, 4, width), f32),
            V((NT, K, width), f32),
            V((tm_n, L, width), jnp.int32),
            V((K, 4 * NT, width), jnp.int32),
            V((K, 4 * NT, width), jnp.int32),
            V((K, 4 * NT, width), f32),
            V((4 * NT, width), f32),
            dma((tm_n,)), dma((tm_n,)), dma((tm_n,)), dma((tm_n,)),
            dma((3,)), dma((3, tm_n)),
            dma((n, 4)), dma((n, 4)),
            dma((n, half)), dma((n, half)),
            dma((5,)),
        ],
        compiler_params=pltpu.CompilerParams(
            collective_id=0, has_side_effects=True, vmem_limit_bytes=40 * 1024 * 1024),
    )(state, far_field, face_index, face_weight, mean_flow)


def solution(mesh):
    dims = (mesh.shape["tm"], mesh.shape["block"] // 2)
    in_specs = (
        P("tm", None, None, "block"),
        P("tm", None, "block"),
        P("tm", "block"),
        P("tm", None, "block"),
        P(),
    )
    out_specs = P("tm", None, None, "block")
    return jax.shard_map(functools.partial(shards, dims), mesh=mesh, in_specs=in_specs,
                         out_specs=out_specs, check_vma=False)
```

```python
import functools
import math

import jax
import jax.numpy as jnp
from jax import lax
from jax.experimental import pallas as pl
from jax.experimental.pallas import tpu as pltpu
from jax.sharding import PartitionSpec as P

SECTION_FACTORS = (0.075, 0.05, 0.1125, 0.15, 0.3)
OMEGA = 1.0
DISSIPATION = 0.2
PAD = 8
MESH = pl.DeviceIdType.MESH


def split_coefficients(count, scale):
    half = count // 2
    d = [0.0] + [0.5 * (-1) ** k / math.tan(math.pi * k / count) for k in range(1, half)] + [0.0]
    even = [0.5 * scale * (d[m] - d[half - m]) for m in range(half)]
    odd = [0.5 * scale * (d[m] + d[half - m]) for m in range(half)]
    even[0] = odd[0] = 0.0
    return even, odd


def time_term(q, even, odd):
    half = len(q) // 2
    quarter = half // 2
    e = [q[n] + q[n + half] for n in range(half)]
    o = [q[n] - q[n + half] for n in range(half)]

    def odd_at(n):
        return (o[n % half], -1.0 if (n // half) % 2 else 1.0)

    low, high = [], []
    for n in range(half):
        ev = None
        od = None
        for m in range(1, quarter):
            term = even[m] * (e[(n - m) % half] - e[(n + m) % half])
            ev = term if ev is None else ev + term
            (a, sa), (b, sb) = odd_at(n - m), odd_at(n + m)
            pair = a - b if sa == sb else a + b
            term = (odd[m] * sa) * pair
            od = term if od is None else od + term
        a, sa = odd_at(n - quarter)
        od = od + (odd[quarter] * sa) * a
        low.append(ev + od)
        high.append(ev - od)
    return low + high


def kernel(dims, state, far, fidx, fw, mf, out, x0, qa, qb, ef, el, rl, ru, cs, cl, cu,
           face, ff, wts, fi, lane_ix, blk_ix, ww, gh,
           in_s, in_r, out_s, out_r, p_s, p_r, h_s, h_r, f_s, f_r, loc):
    tm_n, half, L, R, K = dims
    NT = tm_n * L
    cycle = half * 128
    tiles = R // 8
    nsec = len(SECTION_FACTORS)
    me = lax.axis_index("tm")
    blk = lax.axis_index("block")
    side = lax.div(blk, half)
    place = lax.rem(blk, half)
    row0 = side * half
    lower_b = row0 + lax.rem(place + half - 1, half)
    upper_b = row0 + lax.rem(place + 1, half)
    other0 = (1 - side) * half
    step = 1 - 2 * side
    is_last = me == tm_n - 1
    is_far = me == 0
    rchunk = side * (tm_n - 1) + step * me
    has_lower = rchunk > 0
    has_upper = rchunk < tm_n - 1
    ghost_row = jnp.where(side == 0, PAD + R, PAD - 1)
    far_row = jnp.where(side == 0, PAD - 1, PAD + R)

    def rc(src, dst, ss, rs, dev):
        return pltpu.make_async_remote_copy(src_ref=src, dst_ref=dst, send_sem=ss, recv_sem=rs,
                                            device_id=dev, device_id_type=MESH)

    def rows(p):
        return pl.ds(pl.multiple_of((side * (tm_n - 1) + step * p) * R, R), R)

    def lev(p):
        return pl.ds(p * L, L)

    def peer(t):
        return lax.rem(me + 1 + t, tm_n)

    bar = pltpu.get_barrier_semaphore()

    @pl.loop(0, tm_n - 1)
    def _(t):
        pl.semaphore_signal(bar, inc=1, device_id={"tm": peer(t)}, device_id_type=MESH)

    pl.semaphore_signal(bar, inc=1, device_id={"block": lower_b}, device_id_type=MESH)
    pl.semaphore_signal(bar, inc=1, device_id={"block": upper_b}, device_id_type=MESH)

    @pl.when(is_last)
    def _():
        for h in range(half):
            pl.semaphore_signal(bar, inc=1, device_id={"block": other0 + h}, device_id_type=MESH)

    own = pltpu.make_async_copy(state.at[:, :, rows(me)], x0.at[lev(me)], loc.at[0])
    own.start()
    pl.semaphore_wait(bar, tm_n + 1 + jnp.where(is_last, half, 0))

    def in_copy(p, src_tm):
        return rc(state.at[:, :, rows(p)], x0.at[lev(src_tm)], in_s.at[p], in_r.at[src_tm], {"tm": p})

    @pl.loop(0, tm_n - 1)
    def _(t):
        p = peer(t)
        in_copy(p, me).start()

    def far_copy(src_tm):
        return rc(far, ff.at[lev(src_tm)], p_s.at[0], p_r.at[0, src_tm], {"tm": 0})

    def wt_copy(src_tm):
        return rc(fw, wts.at[lev(src_tm)], p_s.at[1], p_r.at[1, src_tm], {"tm": tm_n - 1})

    def ix_copy(src_tm):
        return rc(fidx, fi.at[src_tm], p_s.at[2], p_r.at[2, src_tm], {"tm": tm_n - 1})

    own_far = pltpu.make_async_copy(far, ff.at[lev(me)], loc.at[1])
    own_wt = pltpu.make_async_copy(fw, wts.at[lev(me)], loc.at[2])
    own_ix = pltpu.make_async_copy(fidx, fi.at[me], loc.at[3])

    @pl.when(is_far)
    def _():
        own_far.start()

    @pl.when(jnp.logical_not(is_far))
    def _():
        far_copy(me).start()

    @pl.when(is_last)
    def _():
        own_wt.start()
        own_ix.start()

    @pl.when(jnp.logical_not(is_last))
    def _():
        wt_copy(me).start()
        ix_copy(me).start()

    lane = lax.broadcasted_iota(jnp.int32, (8, 128), 1)
    lane_pair = jnp.bitwise_or(lane, 1)
    sub = lax.broadcasted_iota(jnp.int32, (8, 128), 0)

    def pack(acc, value, k):
        return jnp.where(lane_pair == k, pltpu.roll(value, k, 1), acc)

    def key(l, v):
        return 2 * (4 * l + v) + 1

    def halo_copies(s):
        low = rc(ef.at[s], ru.at[s], h_s.at[s, 0], h_r.at[s, 0], {"tm": me - step})
        up = rc(el.at[s], rl.at[s], h_s.at[s, 1], h_r.at[s, 1], {"tm": me + step})
        jl = rc(cs.at[s], cu.at[s], h_s.at[s, 2], h_r.at[s, 2], {"block": lower_b})
        ju = rc(cs.at[s], cl.at[s], h_s.at[s, 3], h_r.at[s, 3], {"block": upper_b})
        return low, up, jl, ju

    def face_copy(s, h, edge):
        return rc(edge.at[s], face.at[s, place], f_s.at[s, h], f_r.at[s, place], {"block": other0 + h})

    def face_wait(s, h):
        return rc(ef.at[s], face.at[s, h], f_s.at[s, h], f_r.at[s, h], {"block": other0 + h})

    def send_halos(s):
        low, up, jl, ju = halo_copies(s)

        @pl.when(is_last & (side == 0))
        def _():
            for h in range(half):
                face_copy(s, h, el).start()

        @pl.when(is_last & (side == 1))
        def _():
            for h in range(half):
                face_copy(s, h, ef).start()

        @pl.when(has_lower)
        def _():
            low.start()

        @pl.when(has_upper)
        def _():
            up.start()

        jl.start()
        ju.start()

    def take_level(l, accs):
        accs = list(accs)
        for v in range(4):
            for a in range(tiles):
                value = x0[l, v, pl.ds(8 * a, 8)]
                qa[l, v, pl.ds(PAD + 8 * a, 8)] = value
                accs[a] = pack(accs[a], value, key(l, v))
                if a == 0:
                    ef[0, pl.ds(4 * l + v, 1)] = value[0:1]
                if a == tiles - 1:
                    el[0, pl.ds(4 * l + v, 1)] = value[7:8]
        return tuple(accs)

    own.wait()
    accs = tuple(jnp.zeros((8, 128), jnp.float32) for _ in range(tiles))
    accs = lax.fori_loop(0, L, lambda j, c: take_level(me * L + j, c), accs)

    def arrive(t, c):
        p = peer(tm_n - 2 - t)
        in_copy(p, p).wait_recv()
        return lax.fori_loop(0, L, lambda j, d: take_level(p * L + j, d), c)

    accs = lax.fori_loop(0, tm_n - 1, arrive, accs)
    for a in range(tiles):
        cs[0, pl.ds(8 * a, 8)] = accs[a]
    send_halos(0)

    @pl.when(is_far)
    def _():
        own_far.wait()

        @pl.loop(1, tm_n)
        def _(p):
            far_copy(p).wait_recv()

        @pl.loop(0, NT)
        def _(l):
            for v in range(4):
                row = ff[l, pl.ds(v, 1)]
                qa[l, v, pl.ds(far_row, 1)] = row
                qb[l, v, pl.ds(far_row, 1)] = row

    @pl.when(is_last)
    def _():
        own_wt.wait()
        own_ix.wait()

        @pl.loop(0, tm_n - 1)
        def _(p):
            wt_copy(p).wait_recv()
            ix_copy(p).wait_recv()

        @pl.loop(0, NT // 2)
        def _(m):
            def ix(l):
                return jnp.broadcast_to(fi[lax.div(l, L), pl.ds(lax.rem(l, L), 1)], (8, 128))

            def wt(l, k):
                return jnp.broadcast_to(wts[l, pl.ds(k, 1)], (8, 128))

            start = jnp.where(sub < 4, ix(2 * m), ix(2 * m + 1))
            at = pl.ds(8 * m, 8)
            for k in range(K):
                src = start + k
                src = jnp.where(src >= cycle, src - cycle, src)
                lane_ix[k, at] = jnp.bitwise_and(src, 127)
                blk_ix[k, at] = lax.shift_right_logical(src, 7)
                ww[k, at] = jnp.where(sub < 4, wt(2 * m, k), wt(2 * m + 1, k))

    speed_u = jnp.where(side == 0, mf[0, 0], mf[1, 0])
    speed_v = jnp.where(side == 0, mf[0, 1], mf[1, 1])
    odd_lane = jnp.bitwise_and(lane, 1) == 1
    edge_lane = {0: lane == 0, 127: lane == 127}

    def install(dst, src, at):
        @pl.loop(0, NT)
        def _(l):
            for v in range(4):
                dst[l, v, pl.ds(at, 1)] = src[pl.ds(4 * l + v, 1)]

    def out_copy(q, p, src_tm):
        return rc(q.at[lev(p), :, pl.ds(PAD, R)], out.at[:, :, rows(src_tm)],
                  out_s.at[p], out_r.at[src_tm], {"tm": p})

    for s, factor in enumerate(SECTION_FACTORS):
        q, nq = (qa, qb) if s % 2 == 0 else (qb, qa)
        final = s == nsec - 1
        even, odd = split_coefficients(NT, OMEGA * factor)
        hu, hv, hh = (0.5 * factor) * speed_u, (0.5 * factor) * speed_v, 0.5 * factor

        @pl.loop(0, 4)
        def _(v):
            @pl.loop(0, tiles)
            def _(a):
                at = pl.ds(pl.multiple_of(PAD + 8 * a, 8), 8)
                xs = [q[l, v, at] for l in range(NT)]
                terms = time_term(xs, even, odd)
                for l in range(NT):
                    first = x0[l, v, pl.ds(pl.multiple_of(8 * a, 8), 8)]
                    nq[l, v, at] = first - (terms[l] + (4.0 * DISSIPATION * factor) * xs[l])

        low, up, jl, ju = halo_copies(s)
        jl.wait_recv()
        ju.wait_recv()
        mixed = []
        for a in range(tiles):
            at = pl.ds(8 * a, 8)
            mixed.append(jnp.where(odd_lane, pltpu.roll(cl[s, at], 1, 1), pltpu.roll(cu[s, at], 127, 1)))

        def level(l, accs, which):
            accs = list(accs)
            for slot, a in enumerate(which):
                base = PAD + 8 * a
                di, dj, near = [], [], []
                for v in range(4):
                    x = q[l, v, pl.ds(base, 8)]
                    upx = q[l, v, pl.ds(base + 1, 8)]
                    dnx = q[l, v, pl.ds(base - 1, 8)]
                    border = pltpu.roll(mixed[a], 128 - key(l, v), 1)
                    left = jnp.where(edge_lane[0], border, pltpu.roll(x, 1, 1))
                    right = jnp.where(edge_lane[127], border, pltpu.roll(x, 127, 1))
                    di.append(upx - dnx)
                    dj.append(right - left)
                    near.append((DISSIPATION * factor) * ((upx + dnx) + (right + left)))
                flux = [
                    hu * di[0] + hv * dj[0] + hh * (di[1] + dj[2]),
                    hu * di[1] + hv * dj[1] + hh * di[3],
                    hu * di[2] + hv * dj[2] + hh * dj[3],
                    hu * di[3] + hv * dj[3] + hh * (di[1] + dj[2]),
                ]
                for v in range(4):
                    new = nq[l, v, pl.ds(base, 8)] + (near[v] - flux[v])
                    nq[l, v, pl.ds(base, 8)] = new
                    if not final:
                        accs[slot] = pack(accs[slot], new, key(l, v))
                        if a == 0:
                            ef[s + 1, pl.ds(4 * l + v, 1)] = new[0:1]
                        if a == tiles - 1:
                            el[s + 1, pl.ds(4 * l + v, 1)] = new[7:8]
            return tuple(accs)

        def sweep(which):
            zero = tuple(jnp.zeros((8, 128), jnp.float32) for _ in which)
            step_by = 4 if NT % 4 == 0 else 1

            def several(g, c):
                for j in range(step_by):
                    c = level(step_by * g + j, c, which)
                return c

            accs = lax.fori_loop(0, NT // step_by, several, zero)
            if not final:
                for slot, a in enumerate(which):
                    cs[s + 1, pl.ds(8 * a, 8)] = accs[slot]

        inner = tuple(range(1, tiles - 1))
        outer = tuple(sorted({0, tiles - 1}))
        if inner:
            sweep(inner)

        @pl.when(has_lower)
        def _():
            up.wait_recv()
            install(q, rl.at[s], PAD - 1)

        @pl.when(has_upper)
        def _():
            low.wait_recv()
            install(q, ru.at[s], PAD + R)

        @pl.when(is_last)
        def _():
            for h in range(half):
                face_wait(s, h).wait_recv()

            @pl.loop(0, NT // 2)
            def _(m):
                at = pl.ds(8 * m, 8)
                total = jnp.zeros((8, 128), jnp.float32)
                for k in range(K):
                    picked = jnp.zeros((8, 128), jnp.float32)
                    for h in range(half):
                        got = jnp.take_along_axis(face[s, h, at], lane_ix[k, at], axis=1)
                        picked = jnp.where(blk_ix[k, at] == h, got, picked)
                    total = total + ww[k, at] * picked
                gh[at] = total

            install(q, gh, ghost_row)

        if not final:
            sweep(outer)
            send_halos(s + 1)
        else:
            def finish(t, c):
                p = peer(t)
                for j in range(L):
                    level(p * L + j, (None,) * len(outer), outer)

                @pl.when(t < tm_n - 1)
                def _():
                    out_copy(nq, p, me).start()

                return c

            lax.fori_loop(0, tm_n, finish, 0)
            own_out = pltpu.make_async_copy(nq.at[lev(me), :, pl.ds(PAD, R)], out.at[:, :, rows(me)], loc.at[4])
            own_out.start()

            @pl.loop(0, tm_n - 1)
            def _(t):
                p = peer(t)
                out_copy(nq, p, p).wait_recv()

            own_out.wait()

            @pl.loop(0, tm_n - 1)
            def _(t):
                p = peer(t)
                out_copy(nq, p, me).wait_send()

    @pl.loop(0, tm_n - 1)
    def _(t):
        p = peer(t)
        in_copy(p, me).wait_send()

    @pl.when(jnp.logical_not(is_far))
    def _():
        far_copy(me).wait_send()

    @pl.when(jnp.logical_not(is_last))
    def _():
        wt_copy(me).wait_send()
        ix_copy(me).wait_send()

    for s in range(nsec):
        low, up, jl, ju = halo_copies(s)

        @pl.when(has_lower)
        def _():
            low.wait_send()

        @pl.when(has_upper)
        def _():
            up.wait_send()

        jl.wait_send()
        ju.wait_send()

        @pl.when(is_last)
        def _():
            for h in range(half):
                face_wait(s, h).wait_send()


def shards(dims, state, far_field, face_index, face_weight, mean_flow):
    tm_n, half = dims
    L, _, rows, width = state.shape
    K = face_weight.shape[1]
    R = rows // tm_n
    NT = L * tm_n
    assert width == 128 and NT % 4 == 0 and R % 8 == 0 and 8 * NT <= width
    n = len(SECTION_FACTORS)
    f32 = jnp.float32
    hbm = pl.BlockSpec(memory_space=pl.ANY)
    dma = pltpu.SemaphoreType.DMA
    V = pltpu.VMEM
    return pl.pallas_call(
        functools.partial(kernel, (tm_n, half, L, R, K)),
        out_shape=jax.ShapeDtypeStruct(state.shape, f32),
        in_specs=[hbm, hbm, hbm, hbm, pl.BlockSpec(memory_space=pltpu.SMEM)],
        out_specs=hbm,
        scratch_shapes=[
            V((NT, 4, R, width), f32),
            V((NT, 4, R + 2 * PAD, width), f32),
            V((NT, 4, R + 2 * PAD, width), f32),
            V((n, 4 * NT, width), f32),
            V((n, 4 * NT, width), f32),
            V((n, 4 * NT, width), f32),
            V((n, 4 * NT, width), f32),
            V((n, R, width), f32),
            V((n, R, width), f32),
            V((n, R, width), f32),
            V((n, half, 4 * NT, width), f32),
            V((NT, 4, width), f32),
            V((NT, K, width), f32),
            V((tm_n, L, width), jnp.int32),
            V((K, 4 * NT, width), jnp.int32),
            V((K, 4 * NT, width), jnp.int32),
            V((K, 4 * NT, width), f32),
            V((4 * NT, width), f32),
            dma((tm_n,)), dma((tm_n,)), dma((tm_n,)), dma((tm_n,)),
            dma((3,)), dma((3, tm_n)),
            dma((n, 4)), dma((n, 4)),
            dma((n, half)), dma((n, half)),
            dma((5,)),
        ],
        compiler_params=pltpu.CompilerParams(
            collective_id=0, has_side_effects=True, vmem_limit_bytes=40 * 1024 * 1024),
    )(state, far_field, face_index, face_weight, mean_flow)


def solution(mesh):
    dims = (mesh.shape["tm"], mesh.shape["block"] // 2)
    in_specs = (
        P("tm", None, None, "block"),
        P("tm", None, "block"),
        P("tm", "block"),
        P("tm", None, "block"),
        P(),
    )
    out_specs = P("tm", None, None, "block")
    return jax.shard_map(functools.partial(shards, dims), mesh=mesh, in_specs=in_specs,
                         out_specs=out_specs, check_vma=False)
```
